128 devices in a mesh: shard: 8 (over y, core), model: 16 (over z, x).
Axes of the slice: x: 4, y: 4, z: 4, core: 2. Of those that a mesh axis runs over, the one named last changes fastest.
Arguments:
- train_gate: float32 [4096, 12288], P('shard', 'model'), may hold values from -0.125 to 0.125
- slow_gate: float32 [4096, 12288], P('shard', 'model'), may hold values from -0.09375 to 0.09375
- train_up: float32 [4096, 12288], P('shard', 'model'), may hold values from -0.125 to 0.125
- slow_up: float32 [4096, 12288], P('shard', 'model'), may hold values from -0.09375 to 0.09375
- norm_train: float32 [4096], P(('shard', 'model')), may hold values from 0.25 to 1.75
- norm_step: float32 [4096], P(('shard', 'model')), may hold values from -0.3 to 0.3
Outputs:
- serve_gate: bfloat16 [4096, 12288], P(None, 'model')
- serve_up: bfloat16 [4096, 12288], P(None, 'model')
- factor_gate: float32 [12288], P('model')
- factor_up: float32 [12288], P('model')
- serve_norm: bfloat16 [4096], replicated
- fresh_gate: float32 [4096, 12288], P('shard', 'model')
- fresh_up: float32 [4096, 12288], P('shard', 'model')
The draws below stay inside these ranges and needn't reach their ends.
All inputs are finite; a program needn't handle non-finite values. Where the reference program divides by a largest or mean magnitude, that divisor is 1e-20 or more.
Results may differ from the reference program's by a relative error of at most 0.001.
Values may be sent and summed in bfloat16 or wider, within the bound.
A program may use at most 128 MiB of HBM per device.

```python
import jax
import jax.numpy as jnp

D_MODEL = 4096
D_INNER = 12288


def spiked(result, key, source, target, shards_of, factor):
    owner, partner = [(jnp.arange(result.shape[position]) // (result.shape[position] // shards_of)).reshape([-1 if axis == position else 1 for axis in range(result.ndim)]) for position in (source, target)]
    chosen = jax.random.permutation(key, shards_of)[partner]
    strong = (owner == chosen) | (owner == (partner + shards_of // 2) % shards_of)
    return jnp.where(strong, factor * result, result)


def shard_levels(rng, shape, shards, smallest, high):
    def one(position, shards_of):
        steps = jax.random.uniform(jax.random.fold_in(jax.random.fold_in(rng, 6), position), (shards_of,), jnp.float32, smallest / len(shards), high / len(shards))
        return jnp.repeat(jnp.exp(steps), shape[position] // shards_of).reshape((-1,) + (1,) * (len(shape) - position - 1))

    loudness = one(*shards[0])
    for cut in shards[1:]:
        loudness = loudness * one(*cut)
    return loudness


def noise(rng, dims, width, reach, cuts=(), held_as=jnp.bfloat16):
    factor_of = shard_levels(rng, dims, cuts, -0.22, 0.18) if cuts else 1.0
    drawn = jax.random.normal(rng, dims, jnp.float32) * width * factor_of
    return jnp.minimum(jnp.maximum(drawn, -reach), reach).astype(held_as)


def noise_with(rng, shape, spread, most, shards, heavy, kind=jnp.bfloat16):
    array = spread * jax.random.normal(rng, shape, jnp.float32)
    if shards:
        array = array * shard_levels(rng, shape, shards, -0.22, 0.18)
    return jnp.clip(spiked(array, jax.random.fold_in(rng, 3), *heavy), -most, most).astype(kind)


def setup_inputs(seed: int = 0) -> dict:
    splits = jax.random.split(jax.random.key(seed), 7)
    train_gate = noise_with(splits[0], (D_MODEL, D_INNER), D_MODEL ** -0.5, 0.125, ((0, 8), (1, 16)), (0, 1, 16, 2.0), jnp.float32)
    slow_gate = noise(splits[1], (D_MODEL, D_INNER), D_MODEL ** -0.5, 0.09375, ((0, 8), (1, 16)), jnp.float32)
    train_up = noise_with(splits[2], (D_MODEL, D_INNER), D_MODEL ** -0.5, 0.125, ((0, 8), (1, 16)), (0, 1, 16, 2.0), jnp.float32)
    slow_up = noise(splits[3], (D_MODEL, D_INNER), D_MODEL ** -0.5, 0.09375, ((0, 8), (1, 16)), jnp.float32)
    norm_train = jnp.clip(1.0 + 0.15 * jax.random.normal(splits[4], (D_MODEL,), jnp.float32), 0.25, 1.75)
    norm_step = jnp.clip(jax.random.uniform(splits[5], (D_MODEL,), jnp.float32, -0.3, 0.3) * shard_levels(splits[5], (D_MODEL,), ((0, 128),), -0.4, 0.0), -0.3, 0.3)
    return dict(train_gate=train_gate, slow_gate=slow_gate, train_up=train_up, slow_up=slow_up, norm_train=norm_train, norm_step=norm_step)


keep_rate = 0.75


def reference(train_gate, slow_gate, train_up, slow_up, norm_train, norm_step):
    fresh_gate = keep_rate * slow_gate + (1.0 - keep_rate) * train_gate
    fresh_up = keep_rate * slow_up + (1.0 - keep_rate) * train_up
    factor_gate = jnp.sum(jnp.abs(fresh_gate), axis=0) / D_MODEL
    serve_gate = (fresh_gate / factor_gate).astype(jnp.bfloat16)
    factor_up = jnp.sum(jnp.abs(fresh_up), axis=0) / D_MODEL
    serve_up = (fresh_up / factor_up).astype(jnp.bfloat16)
    serve_norm = (norm_train + norm_step).astype(jnp.bfloat16)
    return serve_gate, serve_up, factor_gate, factor_up, serve_norm, fresh_gate, fresh_up
```

```python
import jax
import jax.numpy as jnp
from jax import lax
from jax.experimental import pallas as pl
from jax.experimental.pallas import tpu as pltpu
from jax.sharding import PartitionSpec as P

KEEP = 0.75
MESH = pl.DeviceIdType.MESH
LANES = 128


def dma(shape=()):
    return pltpu.SemaphoreType.DMA(shape)


def gather_kernel(
    tg, sg, tu, su, nt, ns,
    out_g, out_u, fresh_g, fresh_u, fac_g, fac_u, norm_out,
    stage_t, stage_s, gains, sums0, sums1, norm1, norm2, norm32,
    in_t, in_s, in_n, ex_send, ex_recv, own_send, own_recv, relay_send, relay_recv,
    mate_send, mate_recv, nsend, nrecv,
):
    rows, cols = fresh_g.shape
    per = cols // LANES
    n_blocks = 2 * per
    d_model = out_g.shape[0]
    s = lax.axis_index("shard")
    m = lax.axis_index("model")
    y, c = s // 2, s % 2
    right = ((y + 1) % 4) * 2 + c
    left = ((y + 3) % 4) * 2 + c
    far = ((y + 2) % 4) * 2 + c
    mate = y * 2 + (1 - c)
    z, x = m // 4, m % 4
    source = ((tg, sg), (tu, su))
    fresh = (fresh_g, fresh_u)
    out = (out_g, out_u)
    fac = (fac_g, fac_u)

    def columns(k):
        return k // per, pl.ds((k % per) * LANES, LANES)

    def loads(k):
        a, at = columns(k)
        return (
            pltpu.make_async_copy(source[a][0].at[:, at], stage_t.at[k], in_t.at[k]),
            pltpu.make_async_copy(source[a][1].at[:, at], stage_s.at[k], in_s.at[k]),
        )

    for k in range(n_blocks):
        for copy in loads(k):
            copy.start()
    gain_loads = [
        pltpu.make_async_copy(nt, gains.at[0], in_n.at[0]),
        pltpu.make_async_copy(ns, gains.at[1], in_n.at[1]),
    ]
    for copy in gain_loads:
        copy.start()

    barrier = pltpu.get_barrier_semaphore()
    shard_peers = [(s + d) % 8 for d in range(1, 8)]
    x_peers = [z * 4 + (x + d) % 4 for d in range(1, 4)]
    z_peers = [((z + d) % 4) * 4 + x for d in range(1, 4)]
    for p in shard_peers:
        pl.semaphore_signal(barrier, inc=1, device_id=(p, m), device_id_type=MESH)
    for p in x_peers + z_peers:
        pl.semaphore_signal(barrier, inc=1, device_id=(s, p), device_id_type=MESH)

    def block_sum(k):
        a, at = columns(k)
        for copy in loads(k):
            copy.wait()

        def step(i, total):
            r = pl.multiple_of(i * 64, 64)
            value = KEEP * stage_s[k, pl.ds(r, 64), :] + (1.0 - KEEP) * stage_t[k, pl.ds(r, 64), :]
            fresh[a][pl.ds(r, 64), at] = value
            return total + jnp.sum(jnp.abs(value).reshape(8, 8, LANES), axis=0)

        total = lax.fori_loop(0, rows // 64, step, jnp.zeros((8, LANES), jnp.float32))
        return jnp.sum(total, axis=0, keepdims=True)

    def exchange(g, buffer):
        return [
            pltpu.make_async_remote_copy(
                src_ref=buffer.at[s],
                dst_ref=buffer.at[s],
                send_sem=ex_send.at[g, p],
                recv_sem=ex_recv.at[g, s],
                device_id=(p, m),
                device_id_type=MESH,
            )
            for p in shard_peers
        ]

    def arrivals(g, buffer):
        for p in shard_peers:
            pltpu.make_async_remote_copy(
                src_ref=buffer.at[p],
                dst_ref=buffer.at[p],
                send_sem=ex_send.at[g, p],
                recv_sem=ex_recv.at[g, p],
                device_id=(p, m),
                device_id_type=MESH,
            ).wait_recv()

    def norm_row():
        for copy in gain_loads:
            copy.wait()
        norm1[s] = jnp.zeros((1, LANES), jnp.float32)
        norm1[s, :, 0:32] = gains[0] + gains[1]

    def block_at(k, owner):
        a, at = columns(k)
        return out[a].at[pl.ds(pl.multiple_of(owner * rows, rows), rows), at]

    def sent(k, owner, send, recv, to):
        block = block_at(k, owner)
        return pltpu.make_async_remote_copy(
            src_ref=block,
            dst_ref=block,
            send_sem=send,
            recv_sem=recv,
            device_id=(to, m),
            device_id_type=MESH,
        )

    def own(k, way):
        to = right if way == 0 else left
        return sent(k, s, own_send.at[way, k], own_recv.at[way, k], to)

    def landed(k, way):
        owner = left if way == 0 else right
        return sent(k, owner, own_send.at[way, k], own_recv.at[way, k], right)

    def relay(k, way):
        owner, to = (left, right) if way == 0 else (right, left)
        return sent(k, owner, relay_send.at[k], relay_recv.at[k], to)

    def relayed(k):
        return sent(k, far, relay_send.at[k], relay_recv.at[k], right)

    def to_mate(k, kind):
        owner = (s, left, right, far)[kind]
        return sent(k, owner, mate_send.at[kind, k], mate_recv.at[kind, k], mate)

    def from_mate(k, kind):
        base = (mate, left + 1 - 2 * c, right + 1 - 2 * c, far + 1 - 2 * c)[kind]
        return sent(k, base, mate_send.at[kind, k], mate_recv.at[kind, k], mate)

    def scale(k, row):
        a, at = columns(k)
        factor = row / d_model
        fac[a][k % per : k % per + 1, :] = factor
        inverse = 1.0 / factor
        start = pl.multiple_of(s * rows, rows)

        def step(i, carry):
            r = pl.multiple_of(i * 64, 64)
            value = fresh[a][pl.ds(r, 64), at] * inverse
            out[a][pl.ds(start + r, 64), at] = value.astype(out_g.dtype)
            return carry

        lax.fori_loop(0, rows // 64, step, 0)

    sums0[s] = block_sum(0)
    norm_row()
    pl.semaphore_wait(barrier, 13)
    for copy in exchange(0, sums0):
        copy.start()
    for k in range(1, n_blocks):
        sums1[s, k - 1 : k, :] = block_sum(k)
    for copy in exchange(1, sums1):
        copy.start()

    arrivals(0, sums0)
    row0 = sums0[0]
    for i in range(1, 8):
        row0 = row0 + sums0[i]
    scale(0, row0)
    for way in (0, 1):
        own(0, way).start()
    to_mate(0, 0).start()

    arrivals(1, sums1)
    rest = sums1[0]
    for i in range(1, 8):
        rest = rest + sums1[i]
    right_order = list(range(n_blocks))
    left_order = [0] + list(range(per, n_blocks)) + list(range(1, per))
    scaled = {0}
    for kr, kl in zip(right_order[1:], left_order[1:]):
        for k in (kr, kl):
            if k not in scaled:
                scale(k, rest[k - 1 : k, :])
                scaled.add(k)
        own(kr, 0).start()
        own(kl, 1).start()
        to_mate(kr, 0).start()

    def norm_copy(ref, i, to):
        return pltpu.make_async_remote_copy(
            src_ref=ref,
            dst_ref=ref,
            send_sem=nsend.at[i],
            recv_sem=nrecv.at[i],
            device_id=to,
            device_id_type=MESH,
        )

    for d, p in enumerate(shard_peers):
        norm_copy(norm1.at[s], d, (p, m)).start()
    for d in range(1, 8):
        p = (s + 8 - d) % 8
        norm_copy(norm1.at[p], d - 1, (p, m)).wait_recv()
    lane_row = lax.broadcasted_iota(jnp.int32, (8, LANES), 0)
    tile = jnp.zeros((8, LANES), jnp.float32)
    for i in range(8):
        tile = jnp.where(lane_row == i, norm1[i], tile)
    norm2[m] = tile
    for d, p in enumerate(x_peers):
        norm_copy(norm2.at[m], 7 + d, (s, p)).start()

    for j in range(n_blocks):
        k = right_order[j]
        landed(k, 0).wait_recv()
        if k < per:
            relay(k, 0).start()
        to_mate(k, 1).start()
        k = left_order[j]
        landed(k, 1).wait_recv()
        if k >= per:
            relay(k, 1).start()
        to_mate(k, 2).start()
        if j == 0:
            for d in range(1, 4):
                p = z * 4 + (x + 4 - d) % 4
                norm_copy(norm2.at[p], 6 + d, (s, p)).wait_recv()
            for d, p in enumerate(z_peers):
                norm_copy(norm2.at[pl.ds(z * 4, 4)], 10 + d, (s, p)).start()
        if j == 1:
            for d in range(1, 4):
                pz = (z + 4 - d) % 4
                norm_copy(norm2.at[pl.ds(pz * 4, 4)], 9 + d, (s, pz * 4 + x)).wait_recv()
            for zz in range(4):
                line = norm2[zz * 4]
                for xx in range(1, 4):
                    line = line + pltpu.roll(norm2[zz * 4 + xx], 32 * xx, 1)
                norm32[pl.ds(zz, 8, stride=4), :] = line
            norm_out[...] = norm32[...].astype(norm_out.dtype)

    for j in range(per):
        for k in (j, per + j):
            relayed(k).wait_recv()
            to_mate(k, 3).start()

    for g, buffer in ((0, sums0), (1, sums1)):
        for copy in exchange(g, buffer):
            copy.wait_send()
    for d, p in enumerate(shard_peers):
        norm_copy(norm1.at[s], d, (p, m)).wait_send()
    for d, p in enumerate(x_peers):
        norm_copy(norm2.at[m], 7 + d, (s, p)).wait_send()
    for d, p in enumerate(z_peers):
        norm_copy(norm2.at[pl.ds(z * 4, 4)], 10 + d, (s, p)).wait_send()
    for k in range(n_blocks):
        own(k, 0).wait_send()
        own(k, 1).wait_send()
        relay(k, 0 if k < per else 1).wait_send()
        for kind in range(4):
            to_mate(k, kind).wait_send()
    for k in range(n_blocks):
        for kind in range(4):
            from_mate(k, kind).wait_recv()


def write_kernel(*refs):
    ins, outs, sem = refs[:7], refs[7:14], refs[14]
    copies = []
    for a, b in zip(ins, outs):
        parts = 4 if a.shape[0] % 512 == 0 else 1
        size = a.shape[0] // parts
        for i in range(parts):
            at = pl.ds(i * size, size)
            copies.append(
                pltpu.make_async_copy(a.at[at], b.at[at], sem.at[len(copies)])
            )
    for copy in copies:
        copy.start()
    for copy in copies:
        copy.wait()


def body(tg, sg, tu, su, nt, ns):
    rows, cols = tg.shape
    d_model = rows * 8
    blocks = 2 * cols // LANES
    hbm = pl.BlockSpec(memory_space=pltpu.HBM)
    vmem = pl.BlockSpec(memory_space=pltpu.VMEM)
    shapes = (
        ((d_model, cols), jnp.bfloat16),
        ((d_model, cols), jnp.bfloat16),
        ((rows, cols), jnp.float32),
        ((rows, cols), jnp.float32),
        ((cols // LANES, LANES), jnp.float32),
        ((cols // LANES, LANES), jnp.float32),
        ((32, LANES), jnp.bfloat16),
    )
    given = [
        pltpu.with_memory_space_constraint(a, pltpu.HBM)
        for a in (tg, sg, tu, su, nt.reshape(1, 32), ns.reshape(1, 32))
    ]
    gathered = pl.pallas_call(
        gather_kernel,
        out_shape=[pltpu.VMEM(*a) for a in shapes],
        in_specs=[hbm] * 6,
        out_specs=[vmem] * 7,
        scratch_shapes=[
            pltpu.VMEM((blocks, rows, LANES), jnp.float32),
            pltpu.VMEM((blocks, rows, LANES), jnp.float32),
            pltpu.VMEM((2, 1, 32), jnp.float32),
            pltpu.VMEM((8, 1, LANES), jnp.float32),
            pltpu.VMEM((8, 16, LANES), jnp.float32),
            pltpu.VMEM((8, 1, LANES), jnp.float32),
            pltpu.VMEM((16, 8, LANES), jnp.float32),
            pltpu.VMEM((32, LANES), jnp.float32),
            dma((blocks,)),
            dma((blocks,)),
            dma((2,)),
            dma((2, 8)),
            dma((2, 8)),
            dma((2, blocks)),
            dma((2, blocks)),
            dma((blocks,)),
            dma((blocks,)),
            dma((4, blocks)),
            dma((4, blocks)),
            dma((13,)),
            dma((13,)),
        ],
        compiler_params=pltpu.CompilerParams(
            collective_id=0, has_side_effects=True, vmem_limit_bytes=32 << 20
        ),
    )(*given)
    written = pl.pallas_call(
        write_kernel,
        out_shape=[jax.ShapeDtypeStruct(*a) for a in shapes],
        in_specs=[vmem] * 7,
        out_specs=[hbm] * 7,
        scratch_shapes=[dma((20,))],
        compiler_params=pltpu.CompilerParams(vmem_limit_bytes=16 << 20),
    )(*gathered)
    g, u, fg, fu, cg, cu, norm = written
    return g, u, cg.reshape(cols), cu.reshape(cols), norm.reshape(d_model), fg, fu


def solution(mesh):
    spread = P("shard", "model")
    return jax.shard_map(
        body,
        mesh=mesh,
        in_specs=(spread,) * 4 + (P(("shard", "model")),) * 2,
        out_specs=(
            P(None, "model"), P(None, "model"), P("model"), P("model"), P(), spread, spread,
        ),
        check_vma=False,
    )
```

```python
import jax
import jax.numpy as jnp
from jax import lax
from jax.experimental import pallas as pl
from jax.experimental.pallas import tpu as pltpu
from jax.sharding import PartitionSpec as P

KEEP = 0.75
MESH = pl.DeviceIdType.MESH
LANES = 128
FIRST = 128
UNITS = (
    (0, 0, 512, 0, FIRST),
    (0, 0, 320, FIRST, 768 - FIRST),
    (0, 320, 160, FIRST, 768 - FIRST),
    (0, 480, 32, FIRST, 768 - FIRST),
    (1, 0, 320, 0, 768),
    (1, 320, 160, 0, 768),
    (1, 480, 32, 0, 768),
)
RIGHT, LEFT = (0, 1, 2, 3, 4, 5, 6), (0, 4, 5, 6, 1, 2, 3)
RELAYED_RIGHT, RELAYED_LEFT = (0, 1, 2, 3), (4, 5, 6)


def dma(shape=()):
    return pltpu.SemaphoreType.DMA(shape)


def by_arrival(*queues):
    arrivals = []
    for way, units in queues:
        total = 0
        for u in units:
            total += UNITS[u][2] * UNITS[u][4]
            arrivals.append((total, way, u))
    return [(way, u) for _, way, u in sorted(arrivals)]


def gather_kernel(
    tg, sg, tu, su, nt, ns,
    out_g, out_u, fresh_g, fresh_u, fac_g, fac_u, norm_out,
    stage_g, stage_u, gains, sums0, sums1, norm1, norm2, norm32,
    in_sem, gain_sem, go, ex_send, ex_recv, own_send, own_recv, relay_send, relay_recv,
    mate_send, mate_recv, nsend, nrecv,
):
    rows, cols = fresh_g.shape
    d_model = out_g.shape[0]
    rest = cols - FIRST
    s = lax.axis_index("shard")
    m = lax.axis_index("model")
    y, c = s // 2, s % 2
    right = ((y + 1) % 4) * 2 + c
    left = ((y + 3) % 4) * 2 + c
    far = ((y + 2) % 4) * 2 + c
    mate = y * 2 + (1 - c)
    z, x = m // 4, m % 4
    fresh, out, fac, stage = (fresh_g, fresh_u), (out_g, out_u), (fac_g, fac_u), (stage_g, stage_u)
    shard_peers = [(s + d) % 8 for d in range(1, 8)]
    cross_peers = [z * 4 + (x + d) % 4 for d in range(1, 4)]
    cross_peers += [((z + d) % 4) * 4 + x for d in range(1, 4)]

    barrier = pltpu.get_barrier_semaphore()
    for d in range(1, 4):
        pl.semaphore_signal(
            barrier, inc=1, device_id=(((y + d) % 4) * 2 + 1, m), device_id_type=MESH
        )

    @pl.when(c == 0)
    def _():
        pl.semaphore_signal(barrier, inc=1, device_id=(mate, m), device_id_type=MESH)
        for p in cross_peers:
            pl.semaphore_signal(barrier, inc=1, device_id=(s, p), device_id_type=MESH)

    parts = ((0, 0, rows, 0, FIRST), (0, 0, rows, FIRST, rest), (1, 0, rows // 2, 0, cols), (1, rows // 2, rows // 2, 0, cols))
    for i, (a, r, nr, q, nq) in enumerate(parts):
        for kind, ref in enumerate(((sg, tg), (su, tu))[a]):
            pltpu.make_async_copy(
                ref.at[pl.ds(r, nr), pl.ds(q, nq)],
                stage[a].at[kind, pl.ds(r, nr), pl.ds(q, nq)],
                in_sem.at[i],
            ).start()
    for i, ref in enumerate((nt, ns)):
        pltpu.make_async_copy(ref, gains.at[i], gain_sem).start()

    def settle(ref, sem):
        pltpu.make_async_copy(ref, ref, sem).wait()

    def averaged(i, step, total):
        a, r0, nr, q, nq = parts[i]
        settle(stage[a].at[:, pl.ds(r0, nr), pl.ds(q, nq)], in_sem.at[i])
        at = pl.ds(q, nq)

        def one(j, total):
            r = pl.ds(pl.multiple_of(r0 + j * step, step), step)
            value = KEEP * stage[a][0, r, at] + (1.0 - KEEP) * stage[a][1, r, at]
            fresh[a][r, at] = value
            return total + jnp.sum(jnp.abs(value).reshape(step // 8, 8, nq), axis=0)

        return lax.fori_loop(0, nr // step, one, total)

    def collapsed(total):
        return jnp.sum(total, axis=0, keepdims=True)

    def exchange(g, buffer):
        for p in shard_peers:
            pltpu.make_async_remote_copy(
                src_ref=buffer.at[s],
                dst_ref=buffer.at[s],
                send_sem=ex_send.at[g],
                recv_sem=ex_recv.at[g],
                device_id=(p, m),
                device_id_type=MESH,
            ).start()

    def summed(g, buffer):
        settle(buffer.at[pl.ds(0, 7)], ex_recv.at[g])
        total = buffer[0]
        for i in range(1, 8):
            total = total + buffer[i]
        return total / d_model

    def unit_at(u, owner):
        a, r, nr, q, nq = UNITS[u]
        return out[a].at[pl.ds(pl.multiple_of(owner * rows + r, 32), nr), pl.ds(q, nq)]

    def sent(u, owner, send, recv, to):
        ref = unit_at(u, owner)
        return pltpu.make_async_remote_copy(
            src_ref=ref, dst_ref=ref, send_sem=send, recv_sem=recv, device_id=(to, m), device_id_type=MESH,
        )

    def own(u, way):
        sent(u, s, own_send, own_recv.at[way, u], (right, left)[way]).start()

    def landed(u, way):
        sent(u, (left, right)[way], own_send, own_recv.at[way, u], right).wait_recv()

    def relay(u, way):
        sent(u, (left, right)[way], relay_send, relay_recv.at[u], (right, left)[way]).start()

    def relayed(u):
        sent(u, far, relay_send, relay_recv.at[u], right).wait_recv()

    def to_mate(u, owner):
        sent(u, owner, mate_send, mate_recv, mate).start()

    def scale(u, inverse):
        a, r0, nr, q, nq = UNITS[u]
        at = pl.ds(q, nq)

        def one(j, carry):
            r = pl.multiple_of(r0 + j * 32, 32)
            value = fresh[a][pl.ds(r, 32), at] * inverse
            out[a][pl.ds(pl.multiple_of(s * rows + r, 32), 32), at] = value.astype(out_g.dtype)
            return carry

        lax.fori_loop(0, nr // 32, one, 0)

    def keep_factor(a, q, factor):
        for i in range(factor.shape[1] // LANES):
            k = q // LANES + i
            fac[a][k : k + 1, :] = factor[:, i * LANES : (i + 1) * LANES]

    sums0[s] = collapsed(averaged(0, 64, jnp.zeros((8, FIRST), jnp.float32)))

    @pl.when(c == 1)
    def _():
        pl.semaphore_wait(barrier, 7)
        pl.semaphore_signal(go, inc=1, device_id=(mate, m), device_id_type=MESH)

    @pl.when(c == 0)
    def _():
        pl.semaphore_wait(go, 1)

    exchange(0, sums0)
    sums1[s, :, 0:rest] = collapsed(averaged(1, 32, jnp.zeros((8, rest), jnp.float32)))
    upper = averaged(2, 32, jnp.zeros((8, cols), jnp.float32))
    sums1[s, :, rest : rest + cols] = collapsed(averaged(3, 32, upper))
    exchange(1, sums1)

    factor = summed(0, sums0)
    scale(0, 1.0 / factor)
    own(0, 0)
    own(0, 1)
    to_mate(0, s)
    keep_factor(0, 0, factor)

    factors = summed(1, sums1)
    inverses = 1.0 / factors
    inverse = (inverses[:, 0:rest], inverses[:, rest : rest + cols])
    scaled = {0}
    for ur, ul in zip(RIGHT[1:], LEFT[1:]):
        for way, u in ((0, ur), (1, ul)):
            new = u not in scaled
            if new:
                scale(u, inverse[UNITS[u][0]])
                scaled.add(u)
            own(u, way)
            if new:
                to_mate(u, s)
    keep_factor(0, FIRST, factors[:, 0:rest])
    keep_factor(1, 0, factors[:, rest : rest + cols])

    def norm_copy(ref, i, to):
        return pltpu.make_async_remote_copy(
            src_ref=ref, dst_ref=ref, send_sem=nsend.at[i], recv_sem=nrecv.at[i], device_id=to, device_id_type=MESH,
        )

    settle(gains, gain_sem)
    norm1[s] = jnp.zeros((1, LANES), jnp.float32)
    norm1[s, :, 0:32] = gains[0] + gains[1]
    for d in range(1, 4):
        norm_copy(norm1.at[s], 0, (((y + d) % 4) * 2, m)).start()

    @pl.when(c == 1)
    def _():
        norm_copy(norm1.at[s], 0, (mate, m)).start()

    def norm_along_x():
        settle(norm1.at[pl.ds(0, 7)], nrecv.at[0])
        lane_row = lax.broadcasted_iota(jnp.int32, (8, LANES), 0)
        tile = jnp.zeros((8, LANES), jnp.float32)
        for i in range(8):
            tile = jnp.where(lane_row == i, norm1[i], tile)
        norm2[m] = tile
        pl.semaphore_wait(barrier, 6)
        for p in cross_peers[:3]:
            norm_copy(norm2.at[m], 1, (s, p)).start()

    def norm_along_z():
        settle(norm2.at[pl.ds(0, 3)], nrecv.at[1])
        for p in cross_peers[3:]:
            norm_copy(norm2.at[pl.ds(z * 4, 4)], 2, (s, p)).start()

    def norm_to_mate():
        settle(norm2.at[pl.ds(0, 12)], nrecv.at[2])
        for zz in range(4):
            line = norm2[zz * 4]
            for xx in range(1, 4):
                line = line + pltpu.roll(norm2[zz * 4 + xx], 32 * xx, 1)
            norm32[pl.ds(zz, 8, stride=4), :] = line
        norm_copy(norm32, 3, (mate, m)).start()

    steps = [norm_along_x, norm_along_z, norm_to_mate]
    for i, (way, u) in enumerate(by_arrival((0, RIGHT), (1, LEFT))):
        landed(u, way)
        if u in (RELAYED_RIGHT, RELAYED_LEFT)[way]:
            relay(u, way)
        to_mate(u, (left, right)[way])
        if i % 2 and steps:
            pl.when(c == 0)(steps.pop(0))

    @pl.when(c == 1)
    def _():
        norm_copy(norm32, 3, (mate, m)).wait_recv()
        settle(norm1.at[pl.ds(0, 4)], nsend.at[0])

    @pl.when(c == 0)
    def _():
        settle(norm1.at[pl.ds(0, 3)], nsend.at[0])
        settle(norm2.at[pl.ds(0, 3)], nsend.at[1])
        settle(norm2.at[pl.ds(0, 12)], nsend.at[2])
        norm_copy(norm32, 3, (mate, m)).wait_send()

    norm_out[...] = norm32[...].astype(norm_out.dtype)
    settle(sums0.at[pl.ds(0, 7)], ex_send.at[0])
    settle(sums1.at[pl.ds(0, 7)], ex_send.at[1])

    for _, u in by_arrival((0, RELAYED_RIGHT), (1, RELAYED_LEFT)):
        relayed(u)
        to_mate(u, far)

    settle(out_g.at[pl.ds(0, 4 * rows)], own_send)
    settle(out_g.at[pl.ds(0, 2 * rows)], relay_send)
    settle(out_g, mate_recv)
    settle(out_g, mate_send)


def write_kernel(*refs):
    ins, outs, sem = refs[:7], refs[7:14], refs[14]
    copies = []
    for a, b in zip(ins, outs):
        parts = 4 if a.shape[0] % 512 == 0 else 1
        size = a.shape[0] // parts
        for i in range(parts):
            at = pl.ds(i * size, size)
            pltpu.make_async_copy(a.at[at], b.at[at], sem).start()
    for a, b in zip(ins, outs):
        pltpu.make_async_copy(a, b, sem).wait()


def body(tg, sg, tu, su, nt, ns):
    rows, cols = tg.shape
    d_model = rows * 8
    hbm = pl.BlockSpec(memory_space=pltpu.HBM)
    vmem = pl.BlockSpec(memory_space=pltpu.VMEM)
    shapes = (
        ((d_model, cols), jnp.bfloat16),
        ((d_model, cols), jnp.bfloat16),
        ((rows, cols), jnp.float32),
        ((rows, cols), jnp.float32),
        ((cols // LANES, LANES), jnp.float32),
        ((cols // LANES, LANES), jnp.float32),
        ((32, LANES), jnp.bfloat16),
    )
    given = [
        pltpu.with_memory_space_constraint(a, pltpu.HBM)
        for a in (tg, sg, tu, su, nt.reshape(1, 32), ns.reshape(1, 32))
    ]
    gathered = pl.pallas_call(
        gather_kernel,
        out_shape=[pltpu.VMEM(*a) for a in shapes],
        in_specs=[hbm] * 6,
        out_specs=[vmem] * 7,
        scratch_shapes=[
            pltpu.VMEM((2, rows, cols), jnp.float32),
            pltpu.VMEM((2, rows, cols), jnp.float32),
            pltpu.VMEM((2, 1, 32), jnp.float32),
            pltpu.VMEM((8, 1, FIRST), jnp.float32),
            pltpu.VMEM((8, 1, 2 * cols - FIRST), jnp.float32),
            pltpu.VMEM((8, 1, LANES), jnp.float32),
            pltpu.VMEM((16, 8, LANES), jnp.float32),
            pltpu.VMEM((32, LANES), jnp.float32),
            dma((4,)),
            dma(),
            pltpu.SemaphoreType.REGULAR,
            dma((2,)),
            dma((2,)),
            dma(),
            dma((2, len(UNITS))),
            dma(),
            dma((len(UNITS),)),
            dma(),
            dma(),
            dma((4,)),
            dma((4,)),
        ],
        compiler_params=pltpu.CompilerParams(
            collective_id=0, has_side_effects=True, vmem_limit_bytes=32 << 20
        ),
    )(*given)
    g, u, fg, fu, cg, cu, norm = pl.pallas_call(
        write_kernel,
        out_shape=[jax.ShapeDtypeStruct(*a) for a in shapes],
        in_specs=[vmem] * 7,
        out_specs=[hbm] * 7,
        scratch_shapes=[dma()],
        compiler_params=pltpu.CompilerParams(vmem_limit_bytes=16 << 20),
    )(*gathered)
    return g, u, cg.reshape(cols), cu.reshape(cols), norm.reshape(d_model), fg, fu


def solution(mesh):
    spread = P("shard", "model")
    return jax.shard_map(
        body,
        mesh=mesh,
        in_specs=(spread,) * 4 + (P(("shard", "model")),) * 2,
        out_specs=(
            P(None, "model"), P(None, "model"), P("model"), P("model"), P(), spread, spread,
        ),
        check_vma=False,
    )
```
